32 devices in a mesh: seq: 16 (over z, y, x), head: 2 (over core).
Axes of the slice: x: 2, y: 2, z: 4, core: 2. Of those that a mesh axis runs over, the one named last changes fastest.
Arguments:
- queries: bfloat16 [4096, 32, 128], P('seq', 'head'), may hold values from -192 to 192
- keys: bfloat16 [4096, 8, 128], P(('seq', 'head')), may hold values from -6 to 6
- values: bfloat16 [4096, 8, 128], P(('seq', 'head')), may hold values from -6 to 6
- doc_start: int32 [4096], P('seq'), may hold values from 0 to 4095, as said below
- tile_list: int32 [16, 18], P('seq'), may hold values from 0 to 31, as said below
- tile_count: int32 [16], P('seq'), may hold values from 2 to 18, as said below
Outputs:
- attention_out: bfloat16 [4096, 32, 128], P('seq', 'head')
The draws below stay inside these ranges and needn't reach their ends.
Inputs may be any that keep to these rules, and one draw needn't show every extreme that they name: doc_start never falls, doc_start[i] <= i, and a new document begins at each position where it changes; documents hold 1 to 2048 tokens, one exactly 2048. `tile_list`: row s holds in its first tile_count[s] entries, ascending, exactly the tiles (tile t holds key positions t * 128 to t * 128 + 127) that contain a key visible to some query of positions s * 256 to s * 256 + 255; the later entries equal s * 2. `tile_count`: some row reaches 18.
All inputs are finite; a program needn't handle non-finite values.
Results may differ from the reference program's by a relative error of at most 0.004.
Values may be sent and summed in bfloat16 or wider, within the bound.
A program may use at most 64 MiB of HBM per device.

```python
import jax
import jax.numpy as jnp
from jax import lax

HQ = 32
KVH = 8
HD = 128
TOK_DEV = 256
TILE = 128
MAXDOC = 2048
REACH = 8
MAXT = 18
TOKENS = 4096
N_SEQ = 16


def document_starts(key):
    base_key = jax.random.fold_in(key, 11)
    choose_long = jax.random.randint(jax.random.fold_in(base_key, 1), (TOKENS,), 0, 2)
    short_len = jax.random.randint(jax.random.fold_in(base_key, 2), (TOKENS,), 1, TILE + 1)
    long_len = jax.random.randint(jax.random.fold_in(base_key, 3), (TOKENS,), TILE + 1, MAXDOC + 1)
    lengths = jnp.where(choose_long == 0, short_len, long_len).astype(jnp.int32)
    doc_ends = jnp.cumsum(lengths).astype(jnp.int32)
    start_marks = jnp.zeros((TOKENS,), jnp.int32).at[doc_ends].set(1, mode='drop')
    start_marks = start_marks.at[0].set(1)
    chosen = jax.random.randint(jax.random.fold_in(base_key, 4), (), REACH, N_SEQ).astype(jnp.int32)
    first_pos = chosen * TOK_DEV - MAXDOC + 1
    after_pos = chosen * TOK_DEV + 1
    position = jnp.arange(TOKENS, dtype=jnp.int32)
    inside = (position > first_pos) & (position < after_pos)
    start_marks = jnp.where(inside, 0, start_marks)
    start_marks = jnp.where((position == first_pos) | (position == after_pos), 1, start_marks)
    return lax.cummax(jnp.where(start_marks == 1, position, 0), axis=0).astype(jnp.int32)


def tile_tables(key):
    starts = document_starts(key)
    tiles_own = TOK_DEV // TILE
    first_tile = (starts[::TOK_DEV] // TILE).astype(jnp.int32)
    own_first = jnp.arange(N_SEQ, dtype=jnp.int32) * tiles_own
    slot_ids = jnp.arange(MAXT, dtype=jnp.int32)
    live_count = own_first + tiles_own - first_tile
    listed = first_tile[:, None] + slot_ids[None, :]
    listed = jnp.where(slot_ids[None, :] < live_count[:, None], listed, own_first[:, None])
    return (listed.astype(jnp.int32), live_count.astype(jnp.int32))


def attention_draws(key):
    base_key = jax.random.fold_in(key, 23)
    keys_raw = jax.random.truncated_normal(jax.random.fold_in(base_key, 1), -6.0, 6.0, (TOKENS, KVH, HD), jnp.float32)
    queries_raw = jax.random.truncated_normal(jax.random.fold_in(base_key, 2), -6.0, 6.0, (TOKENS, HQ, HD), jnp.float32)
    return (queries_raw, keys_raw)


def draw_queries(key, part):
    return attention_draws(key)[0].astype(jnp.bfloat16)


def draw_keys(key, part):
    return attention_draws(key)[1].astype(jnp.bfloat16)


def draw_doc_start(key, part):
    return document_starts(key)


def draw_tile_list(key, part):
    return tile_tables(key)[0]


def draw_tile_count(key, part):
    return tile_tables(key)[1]


def block_levels(rng, dims, cuts, low, high):
    level, own = 1.0, jax.random.fold_in(rng, 6)
    for dim, shards_of in cuts:
        draws = jnp.exp(jax.random.uniform(jax.random.fold_in(own, dim), (shards_of,), jnp.float32, low / len(cuts), high / len(cuts)))
        level = level * jnp.repeat(draws, dims[dim] // shards_of).reshape([-1 if axis == dim else 1 for axis in range(len(dims))])
    return level


def noise(own_key, shape, spread, reach, split=(), held_as=jnp.bfloat16):
    array = jax.random.normal(own_key, shape, jnp.float32) * spread
    if len(split) > 0:
        array = block_levels(own_key, shape, split, -0.22, 0.18) * array
    return jnp.clip(array, min=-reach, max=reach).astype(held_as)


def setup_inputs(seed: int = 0) -> dict:
    splits = jax.random.split(jax.random.key(seed), 7)
    queries = draw_queries(jax.random.fold_in(splits[6], 71), 0)
    keys = draw_keys(jax.random.fold_in(splits[6], 71), 0)
    values = noise(splits[2], (TOKENS, KVH, HD), 1.0, 6.0, ((0, 32),))
    doc_start = draw_doc_start(jax.random.fold_in(splits[6], 71), 0)
    tile_list = draw_tile_list(jax.random.fold_in(splits[6], 71), 0)
    tile_count = draw_tile_count(jax.random.fold_in(splits[6], 71), 0)
    return dict(queries=queries, keys=keys, values=values, doc_start=doc_start, tile_list=tile_list, tile_count=tile_count)


def reference(queries, keys, values, doc_start, tile_list, tile_count):
    group_size = HQ // KVH
    score_scale = 1.0 / (HD ** 0.5)
    key_tiles = keys.reshape(TOKENS // TILE, TILE, KVH, HD)
    value_tiles = values.reshape(TOKENS // TILE, TILE, KVH, HD)

    def one_shard(shard_index):
        query_block = lax.dynamic_slice_in_dim(queries, (shard_index * TOK_DEV).astype(jnp.int32), TOK_DEV, 0)
        starts = lax.dynamic_slice_in_dim(doc_start, (shard_index * TOK_DEV).astype(jnp.int32), TOK_DEV, 0)
        listed = tile_list[shard_index]
        live_count = tile_count[shard_index]
        key_block = key_tiles[listed].reshape(MAXT * TILE, KVH, HD)
        value_block = value_tiles[listed].reshape(MAXT * TILE, KVH, HD)
        key_pos = (listed[:, None] * TILE + jnp.arange(TILE, dtype=jnp.int32)[None, :]).reshape(-1)
        live_slot = jnp.repeat(jnp.arange(MAXT, dtype=jnp.int32) < live_count, TILE)
        query_pos = (shard_index * TOK_DEV).astype(jnp.int32) + jnp.arange(TOK_DEV, dtype=jnp.int32)
        visible = (key_pos[None, :] >= starts[:, None]) & (key_pos[None, :] <= query_pos[:, None]) & live_slot[None, :]
        grouped = query_block.reshape(TOK_DEV, KVH, group_size, HD).astype(jnp.float32)
        scores = jnp.einsum("tgch,kgh->gctk", grouped, key_block.astype(jnp.float32)) * score_scale
        scores = jnp.where(visible[None, None], scores, -jnp.inf)
        row_top = jnp.max(scores, axis=-1, keepdims=True)
        weights = jnp.where(visible[None, None], jnp.exp(scores - row_top), jnp.float32(0.0))
        weight_sum = jnp.sum(weights, axis=-1)
        rounded = lax.optimization_barrier(weights.astype(jnp.bfloat16)).astype(jnp.float32)
        summed = jnp.einsum("gctk,kgh->gcth", rounded, value_block.astype(jnp.float32))
        result = summed / weight_sum[..., None]
        result = jnp.transpose(result, (2, 0, 1, 3)).reshape(TOK_DEV, HQ, HD)
        return result.astype(jnp.bfloat16)

    blocks = lax.map(one_shard, jnp.arange(N_SEQ, dtype=jnp.int32))
    return blocks.reshape(TOKENS, HQ, HD)
```

```python
import functools

import jax
import jax.numpy as jnp
from jax import lax
from jax.experimental import pallas as pl
from jax.experimental.pallas import tpu as pltpu
from jax.sharding import PartitionSpec as P

TILE = 128
MAXDOC = 2048
PLANE = 4
LOG2E = 1.4426950408889634
NEGATIVE = -1e30
FAR = 1 << 24


def kernel(groups, levels, rel_ref, q_ref, k_ref, v_ref, o_ref, kbuf, vbuf, top, total, acc,
           local_sem, partner_send, own_send, relay_send, recv):
    me = lax.axis_index("seq")
    core = lax.axis_index("head")
    z, p = me // PLANE, me % PLANE
    side = p % 2
    px = p + 1 - 2 * side
    py = p + 2 - 4 * (p // 2)
    pd = PLANE - 1 - p
    base = z * PLANE
    last = groups - 1
    heads = kbuf.shape[1]
    q_heads = q_ref.shape[0]
    group_size = q_heads // heads
    tile = k_ref.shape[1]
    tokens = kbuf.shape[2]
    scale = LOG2E * q_ref.shape[-1] ** (-0.5)
    residue = {"own": p, "x": px, "y": py, "diag": pd}
    bufs = (kbuf, vbuf)

    def where_to(seq):
        return {"seq": seq, "head": core}

    barrier = pltpu.get_barrier_semaphore()
    pl.semaphore_signal(barrier, inc=1, device_id={"seq": me, "head": 1 - core},
                        device_id_type=pl.DeviceIdType.MESH)
    for mate in (px, py):
        pl.semaphore_signal(barrier, inc=1, device_id=where_to(base + mate),
                            device_id_type=pl.DeviceIdType.MESH)

    @pl.when(z < last)
    def _():
        pl.semaphore_signal(barrier, inc=1, device_id=where_to(me + PLANE),
                            device_id_type=pl.DeviceIdType.MESH)

    @pl.when(z > 0)
    def _():
        pl.semaphore_signal(barrier, inc=1, device_id=where_to(me - PLANE),
                            device_id_type=pl.DeviceIdType.MESH)

    pl.semaphore_wait(barrier, 3 + jnp.minimum(last - z, 1) + jnp.minimum(z, 1))

    mine = pl.multiple_of(core * tile, tile)
    theirs = pl.multiple_of((1 - core) * tile, tile)
    first_slot = p
    own_parts = (
        (k_ref, kbuf.at[first_slot, :, pl.ds(mine, tile), :]),
        (v_ref, vbuf.at[first_slot, :, :, pl.ds(mine, tile)]),
    )
    partner = []
    local = []
    for which in range(2):
        src, dst = own_parts[which]
        copy = pltpu.make_async_remote_copy(
            src_ref=src.at[pl.ds((1 - core) * heads, heads)],
            dst_ref=dst,
            send_sem=partner_send.at[which],
            recv_sem=recv.at[which, first_slot],
            device_id={"seq": me, "head": 1 - core},
            device_id_type=pl.DeviceIdType.MESH,
        )
        copy.start()
        partner.append(copy)
        copy = pltpu.make_async_copy(src.at[pl.ds(core * heads, heads)], dst, local_sem.at[which])
        copy.start()
        local.append(copy)

    def needs(level, r, dst):
        if level == 0:
            return r < dst
        if level == levels:
            return r > dst
        return dst >= 0

    pending = []

    def send(condition, which, level, r, to_level, seq, sem):
        copy = pltpu.make_async_remote_copy(
            src_ref=bufs[which].at[level * PLANE + r],
            dst_ref=bufs[which].at[to_level * PLANE + r],
            send_sem=sem,
            recv_sem=recv.at[which, to_level * PLANE + r],
            device_id=where_to(seq),
            device_id_type=pl.DeviceIdType.MESH,
        )
        pl.when(condition)(copy.start)
        pending.append((condition, copy))

    def have(level, origin):
        held = z >= level
        if origin != "own":
            held = held & needs(level, residue[origin], p)
        return held

    def arrive(level, origin, which):
        r = residue[origin]
        slot = level * PLANE + r
        here = have(level, origin)

        if level == 0 and origin == "own":
            partner[which].wait_recv()
            local[which].wait()
        else:
            @pl.when(here)
            def _():
                pltpu.make_async_remote_copy(
                    src_ref=bufs[which].at[slot],
                    dst_ref=bufs[which].at[slot],
                    send_sem=own_send.at[0, 0, 0],
                    recv_sem=recv.at[which, slot],
                    device_id=where_to(base + px),
                    device_id_type=pl.DeviceIdType.MESH,
                ).wait_recv()

        if origin == "own":
            if level < levels:
                send(here & (z < last), which, level, r, level + 1, me + PLANE, own_send.at[0, level, which])
            send(here & needs(level, p, px), which, level, r, level, base + px, own_send.at[1, level, which])
            send(here & needs(level, p, py), which, level, r, level, base + py, own_send.at[2, level, which])
        elif origin == "x":
            if which == 1:
                go = here & needs(level, px, py)
                if level in (0, levels):
                    go = go & ((px == 0) | (px == PLANE - 1))
                send(go, which, level, r, level, base + py, relay_send.at[0, level, which])
        elif origin == "y":
            go = here & needs(level, py, px)
            if which == 1:
                if level in (0, levels):
                    go = go & (py != 0) & (py != PLANE - 1)
                else:
                    go = None
            if go is not None:
                send(go, which, level, r, level, base + px, relay_send.at[1, level, which])

    def mask_of(slot, causal):
        keys = lax.broadcasted_iota(jnp.int32, (tile, tokens), 0)
        parts = []
        for half in range(tokens // tile):
            part = keys >= rel_ref[pl.ds(slot * (tokens // tile) + half, 1), :]
            if causal:
                part = part & (keys + half * tile <= lax.broadcasted_iota(jnp.int32, (tile, tokens), 1))
            parts.append(part)
        return jnp.concatenate([jnp.where(part, 0.0, NEGATIVE) for part in parts], axis=0)

    def compute(slot, first):
        def one_head(g, _):
            k_tile = kbuf[slot, g]
            v_tile = vbuf[slot, g]
            bias = mask_of(slot, first)
            for c in range(group_size):
                h = g * group_size + c
                scores = lax.dot_general(k_tile, q_ref[h], (((1,), (1,)), ((), ())),
                                         preferred_element_type=jnp.float32)
                scores = scores + bias
                new_top = jnp.max(scores, axis=0, keepdims=True)
                if not first:
                    old_top = top[h]
                    new_top = jnp.maximum(old_top, new_top)
                    factor = jnp.exp2((old_top - new_top) * scale)
                weights = jnp.exp2((scores - new_top) * scale)
                weight_sum = jnp.sum(weights, axis=0, keepdims=True)
                summed = lax.dot_general(v_tile, weights.astype(jnp.bfloat16), (((1,), (0,)), ((), ())),
                                         preferred_element_type=jnp.float32)
                top[h] = new_top
                if first:
                    total[h] = weight_sum
                    acc[h] = summed
                else:
                    total[h] = total[h] * factor + weight_sum
                    acc[h] = acc[h] * factor + summed
            return 0

        lax.fori_loop(0, heads, one_head, 0)

    stages = [[(0, "own")], [(1, "own"), (0, "x"), (0, "y")]]
    stages.append([(0, "diag"), (1, "x"), (1, "y"), (2, "own")])
    stages.append([(1, "diag"), (2, "x"), (2, "y")])
    stages.append([(2, "diag")])
    for stage in stages:
        for which in range(2):
            for level, origin in stage:
                arrive(level, origin, which)
        for level, origin in stage:
            slot = level * PLANE + residue[origin]
            if level == 0 and origin == "own":
                compute(slot, True)
            else:
                pl.when(have(level, origin))(functools.partial(compute, slot, False))

    def finish(h, _):
        o_ref[h] = jnp.transpose(acc[h] / total[h]).astype(o_ref.dtype)
        return 0

    lax.fori_loop(0, q_heads, finish, 0)
    for copy in partner:
        copy.wait_send()
    for condition, copy in pending:
        pl.when(condition)(copy.wait_send)


def body(groups, queries, keys, values, doc_start, tile_list, tile_count):
    tokens, q_heads, dim = queries.shape
    tile, all_heads, _ = keys.shape
    heads = all_heads // lax.axis_size("head")
    levels = MAXDOC // tokens // PLANE
    slots = (levels + 1) * PLANE
    halves = tokens // tile
    z = lax.axis_index("seq") // PLANE
    slot = jnp.arange(slots, dtype=jnp.int32)
    block = (z - slot // PLANE) * PLANE + slot % PLANE
    ids = (block[:, None] * halves + jnp.arange(halves, dtype=jnp.int32)).reshape(-1)
    live = jnp.arange(tile_list.shape[1], dtype=jnp.int32) < tile_count[0]
    listed = jnp.any((tile_list[0][None, :] == ids[:, None]) & live[None, :], axis=1)
    rel = jnp.where(listed[:, None], doc_start[None, :] - ids[:, None] * tile, FAR)

    vmem = pl.BlockSpec(memory_space=pltpu.VMEM)
    out = pl.pallas_call(
        functools.partial(kernel, groups, levels),
        out_shape=jax.ShapeDtypeStruct((q_heads, tokens, dim), queries.dtype),
        in_specs=[vmem] * 4,
        out_specs=vmem,
        scratch_shapes=[
            pltpu.VMEM((slots, heads, tokens, dim), keys.dtype),
            pltpu.VMEM((slots, heads, dim, tokens), values.dtype),
            pltpu.VMEM((q_heads, 1, tokens), jnp.float32),
            pltpu.VMEM((q_heads, 1, tokens), jnp.float32),
            pltpu.VMEM((q_heads, dim, tokens), jnp.float32),
            pltpu.SemaphoreType.DMA((2,)),
            pltpu.SemaphoreType.DMA((2,)),
            pltpu.SemaphoreType.DMA((3, levels + 1, 2)),
            pltpu.SemaphoreType.DMA((2, levels + 1, 2)),
            pltpu.SemaphoreType.DMA((2, slots)),
        ],
        compiler_params=pltpu.CompilerParams(
            collective_id=0, has_side_effects=True, vmem_limit_bytes=40 * 1024 * 1024),
    )(rel, queries.transpose(1, 0, 2), keys.transpose(1, 0, 2), values.transpose(1, 2, 0))
    return out.transpose(1, 0, 2)


def solution(mesh):
    in_specs = (
        P("seq", "head", None),
        P(("seq", "head"), None, None),
        P(("seq", "head"), None, None),
        P("seq"),
        P("seq", None),
        P("seq"),
    )
    return jax.shard_map(
        functools.partial(body, mesh.shape["seq"] // PLANE),
        mesh=mesh, in_specs=in_specs, out_specs=P("seq", "head", None), check_vma=False)
```

```python
import functools

import jax
import jax.numpy as jnp
from jax import lax
from jax.experimental import pallas as pl
from jax.experimental.pallas import tpu as pltpu
from jax.sharding import PartitionSpec as P

TILE = 128
MAXDOC = 2048
PLANE = 4
LOG2E = 1.4426950408889634
NEGATIVE = -1e30
FAR = 1 << 24


def kernel(groups, levels, rel_ref, q_ref, kv_ref, o_ref, buf, top, total, acc,
           local_sem, partner_send, own_send, relay_send, recv):
    me = lax.axis_index("seq")
    core = lax.axis_index("head")
    z, p = me // PLANE, me % PLANE
    side = p % 2
    px = p + 1 - 2 * side
    py = p + 2 - 4 * (p // 2)
    pd = PLANE - 1 - p
    base = z * PLANE
    last = groups - 1
    heads = buf.shape[1]
    q_heads = q_ref.shape[0]
    group_size = q_heads // heads
    tile = kv_ref.shape[2]
    tokens = buf.shape[3]
    scale = LOG2E * q_ref.shape[-1] ** (-0.5)
    residue = {"own": p, "x": px, "y": py, "diag": pd}
    split = heads // 2

    def where_to(seq):
        return {"seq": seq, "head": core}

    barrier = pltpu.get_barrier_semaphore()
    pl.semaphore_signal(barrier, inc=1, device_id={"seq": me, "head": 1 - core},
                        device_id_type=pl.DeviceIdType.MESH)
    for mate in (px, py):
        pl.semaphore_signal(barrier, inc=1, device_id=where_to(base + mate),
                            device_id_type=pl.DeviceIdType.MESH)

    @pl.when(z < last)
    def _():
        pl.semaphore_signal(barrier, inc=1, device_id=where_to(me + PLANE),
                            device_id_type=pl.DeviceIdType.MESH)

    @pl.when(z > 0)
    def _():
        pl.semaphore_signal(barrier, inc=1, device_id=where_to(me - PLANE),
                            device_id_type=pl.DeviceIdType.MESH)

    pl.semaphore_wait(barrier, 3 + jnp.minimum(last - z, 1) + jnp.minimum(z, 1))

    mine = pl.multiple_of(core * tile, tile)
    own_part = buf.at[p, :, :, pl.ds(mine, tile), :]
    partner = pltpu.make_async_remote_copy(
        src_ref=kv_ref.at[pl.ds((1 - core) * heads, heads)],
        dst_ref=own_part,
        send_sem=partner_send,
        recv_sem=recv.at[p, 0],
        device_id={"seq": me, "head": 1 - core},
        device_id_type=pl.DeviceIdType.MESH,
    )
    partner.start()
    local = pltpu.make_async_copy(kv_ref.at[pl.ds(core * heads, heads)], own_part, local_sem)
    local.start()

    def needs(level, r, dst):
        if level == 0:
            return r < dst
        if level == levels:
            return r > dst
        return dst >= 0

    def sends(level, origin, g):
        r = residue[origin]
        slot = level * PLANE + r
        here = have(level, origin)

        def copy(to_level, seq, sem):
            return pltpu.make_async_remote_copy(
                src_ref=buf.at[slot, g],
                dst_ref=buf.at[to_level * PLANE + r, g],
                send_sem=sem,
                recv_sem=recv.at[to_level * PLANE + r, g],
                device_id=where_to(seq),
                device_id_type=pl.DeviceIdType.MESH,
            )

        found = []
        if origin == "own":
            if level < levels:
                found.append((here & (z < last), copy(level + 1, me + PLANE, own_send.at[0, level, g])))
            found.append((here & needs(level, p, px), copy(level, base + px, own_send.at[1, level, g])))
            found.append((here & needs(level, p, py), copy(level, base + py, own_send.at[2, level, g])))
        elif origin == "x":
            go = here & needs(level, px, py) & (g >= split)
            if level in (0, levels):
                go = go & ((px == 0) | (px == PLANE - 1))
            found.append((go, copy(level, base + py, relay_send.at[0, level, g])))
        elif origin == "y":
            go = here & needs(level, py, px)
            if level in (0, levels):
                go = go & ((g < split) | ((py != 0) & (py != PLANE - 1)))
            else:
                go = go & (g < split)
            found.append((go, copy(level, base + px, relay_send.at[1, level, g])))
        return found

    def have(level, origin):
        held = z >= level
        if origin != "own":
            held = held & needs(level, residue[origin], p)
        return held

    def arrive(level, origin, g):
        if (level, origin) != (0, "own"):
            slot = level * PLANE + residue[origin]

            @pl.when(have(level, origin))
            def _():
                pltpu.make_async_remote_copy(
                    src_ref=buf.at[slot, g],
                    dst_ref=buf.at[slot, g],
                    send_sem=own_send.at[0, 0, 0],
                    recv_sem=recv.at[slot, g],
                    device_id=where_to(base + px),
                    device_id_type=pl.DeviceIdType.MESH,
                ).wait_recv()

        for condition, copy in sends(level, origin, g):
            pl.when(condition)(copy.start)

    def mask_of(slot, causal):
        keys = lax.broadcasted_iota(jnp.int32, (tile, tokens), 0)
        parts = []
        for half in range(tokens // tile):
            part = keys >= rel_ref[pl.ds(slot * (tokens // tile) + half, 1), :]
            if causal:
                part = part & (keys + half * tile <= lax.broadcasted_iota(jnp.int32, (tile, tokens), 1))
            parts.append(part)
        return jnp.concatenate([jnp.where(part, 0.0, NEGATIVE) for part in parts], axis=0)

    def compute(slot, g, first):
        k_tile = buf[slot, g, 0]
        v_tile = jnp.concatenate(
            [buf[slot, g, 1, half * tile:(half + 1) * tile] for half in range(tokens // tile)], axis=1)
        bias = mask_of(slot, first)
        for c in range(group_size):
            h = g * group_size + c
            scores = lax.dot_general(k_tile, q_ref[h], (((1,), (1,)), ((), ())),
                                     preferred_element_type=jnp.float32)
            scores = scores + bias
            new_top = jnp.max(scores, axis=0, keepdims=True)
            if not first:
                old_top = top[h]
                new_top = jnp.maximum(old_top, new_top)
                factor = jnp.exp2((old_top - new_top) * scale)
            weights = jnp.exp2((scores - new_top) * scale)
            weight_sum = jnp.sum(weights, axis=0, keepdims=True)
            summed = lax.dot_general(v_tile, weights.astype(jnp.bfloat16), (((1,), (0,)), ((), ())),
                                     preferred_element_type=jnp.float32)
            top[h] = new_top
            if first:
                total[h] = weight_sum
                acc[h] = summed
            else:
                total[h] = total[h] * factor + weight_sum
                acc[h] = acc[h] * factor + summed

    partner.wait_recv()
    local.wait()
    stages = [
        [(0, "own")],
        [(1, "own"), (0, "x"), (0, "y")],
        [(1, "x"), (1, "y"), (0, "diag"), (2, "own")],
        [(1, "diag"), (2, "x"), (2, "y")],
        [(2, "diag")],
    ]
    everything = [entry for stage in stages for entry in stage]

    def start_own(g, _):
        arrive(0, "own", g)
        return 0

    lax.fori_loop(0, heads, start_own, 0)
    for stage in stages:
        def one_head(g, _):
            for level, origin in stage:
                slot = level * PLANE + residue[origin]
                if (level, origin) == (0, "own"):
                    compute(slot, g, True)
            if stage[0] != (0, "own"):
                for level, origin in stage:
                    arrive(level, origin, g)
                for level, origin in stage:
                    slot = level * PLANE + residue[origin]
                    pl.when(have(level, origin))(functools.partial(compute, slot, g, False))
            return 0

        lax.fori_loop(0, heads, one_head, 0)

    def finish(h, _):
        o_ref[h] = jnp.transpose(acc[h] / total[h]).astype(o_ref.dtype)
        return 0

    lax.fori_loop(0, q_heads, finish, 0)
    partner.wait_send()

    def sent(g, _):
        for level, origin in everything:
            for condition, copy in sends(level, origin, g):
                pl.when(condition)(copy.wait_send)
        return 0

    lax.fori_loop(0, heads, sent, 0)


def body(groups, queries, keys, values, doc_start, tile_list, tile_count):
    tokens, q_heads, dim = queries.shape
    tile, all_heads, _ = keys.shape
    heads = all_heads // lax.axis_size("head")
    levels = MAXDOC // tokens // PLANE
    slots = (levels + 1) * PLANE
    halves = tokens // tile
    z = lax.axis_index("seq") // PLANE
    slot = jnp.arange(slots, dtype=jnp.int32)
    block = (z - slot // PLANE) * PLANE + slot % PLANE
    ids = (block[:, None] * halves + jnp.arange(halves, dtype=jnp.int32)).reshape(-1)
    live = jnp.arange(tile_list.shape[1], dtype=jnp.int32) < tile_count[0]
    listed = jnp.any((tile_list[0][None, :] == ids[:, None]) & live[None, :], axis=1)
    rel = jnp.where(listed[:, None], doc_start[None, :] - ids[:, None] * tile, FAR)

    vmem = pl.BlockSpec(memory_space=pltpu.VMEM)
    out = pl.pallas_call(
        functools.partial(kernel, groups, levels),
        out_shape=jax.ShapeDtypeStruct((q_heads, tokens, dim), queries.dtype),
        in_specs=[vmem] * 3,
        out_specs=vmem,
        scratch_shapes=[
            pltpu.VMEM((slots, heads, 2, tokens, dim), keys.dtype),
            pltpu.VMEM((q_heads, 1, tokens), jnp.float32),
            pltpu.VMEM((q_heads, 1, tokens), jnp.float32),
            pltpu.VMEM((q_heads, dim, tokens), jnp.float32),
            pltpu.SemaphoreType.DMA,
            pltpu.SemaphoreType.DMA,
            pltpu.SemaphoreType.DMA((3, levels + 1, heads)),
            pltpu.SemaphoreType.DMA((2, levels + 1, heads)),
            pltpu.SemaphoreType.DMA((slots, heads)),
        ],
        compiler_params=pltpu.CompilerParams(
            collective_id=0, has_side_effects=True, vmem_limit_bytes=40 * 1024 * 1024),
    )(rel, queries.transpose(1, 0, 2), jnp.stack([keys.transpose(1, 0, 2), values.transpose(1, 2, 0)], axis=1))
    return out.transpose(1, 0, 2)


def solution(mesh):
    in_specs = (
        P("seq", "head", None),
        P(("seq", "head"), None, None),
        P(("seq", "head"), None, None),
        P("seq"),
        P("seq", None),
        P("seq"),
    )
    return jax.shard_map(
        functools.partial(body, mesh.shape["seq"] // PLANE),
        mesh=mesh, in_specs=in_specs, out_specs=P("seq", "head", None), check_vma=False)
```

```python
import functools

import jax
import jax.numpy as jnp
from jax import lax
from jax.experimental import pallas as pl
from jax.experimental.pallas import tpu as pltpu
from jax.sharding import PartitionSpec as P

TILE = 128
MAXDOC = 2048
PLANE = 4
LOG2E = 1.4426950408889634
NEGATIVE = -1e30
FAR = 1 << 24


def kernel(groups, levels, rel_ref, q_ref, kv_ref, o_ref, buf, top, total, acc,
           local_sem, partner_send, own_send, relay_send, recv):
    me = lax.axis_index("seq")
    core = lax.axis_index("head")
    z, p = me // PLANE, me % PLANE
    side = p % 2
    px = p + 1 - 2 * side
    py = p + 2 - 4 * (p // 2)
    pd = PLANE - 1 - p
    base = z * PLANE
    last = groups - 1
    heads = buf.shape[1]
    q_heads = q_ref.shape[0]
    group_size = q_heads // heads
    tile = kv_ref.shape[2]
    tokens = buf.shape[3]
    scale = LOG2E * q_ref.shape[-1] ** (-0.5)
    residue = {"own": p, "x": px, "y": py, "diag": pd}
    split = heads // 2

    def where_to(seq):
        return {"seq": seq, "head": core}

    barrier = pltpu.get_barrier_semaphore()
    pl.semaphore_signal(barrier, inc=1, device_id={"seq": me, "head": 1 - core},
                        device_id_type=pl.DeviceIdType.MESH)
    for mate in (px, py):
        pl.semaphore_signal(barrier, inc=1, device_id=where_to(base + mate),
                            device_id_type=pl.DeviceIdType.MESH)

    @pl.when(z < last)
    def _():
        pl.semaphore_signal(barrier, inc=1, device_id=where_to(me + PLANE),
                            device_id_type=pl.DeviceIdType.MESH)

    @pl.when(z > 0)
    def _():
        pl.semaphore_signal(barrier, inc=1, device_id=where_to(me - PLANE),
                            device_id_type=pl.DeviceIdType.MESH)

    pl.semaphore_wait(barrier, 3 + jnp.minimum(last - z, 1) + jnp.minimum(z, 1))

    mine = pl.multiple_of(core * tile, tile)
    own_part = buf.at[p, :, :, pl.ds(mine, tile), :]
    partner = pltpu.make_async_remote_copy(
        src_ref=kv_ref.at[pl.ds((1 - core) * heads, heads)],
        dst_ref=own_part,
        send_sem=partner_send,
        recv_sem=recv.at[p, 0],
        device_id={"seq": me, "head": 1 - core},
        device_id_type=pl.DeviceIdType.MESH,
    )
    partner.start()
    local = pltpu.make_async_copy(kv_ref.at[pl.ds(core * heads, heads)], own_part, local_sem)
    local.start()

    def needs(level, r, dst):
        if level == 0:
            return r < dst
        if level == levels:
            return r > dst
        return dst >= 0

    def sends(level, origin, g):
        r = residue[origin]
        slot = level * PLANE + r
        here = have(level, origin)

        def copy(to_level, seq, sem):
            return pltpu.make_async_remote_copy(
                src_ref=buf.at[slot, g],
                dst_ref=buf.at[to_level * PLANE + r, g],
                send_sem=sem,
                recv_sem=recv.at[to_level * PLANE + r, g],
                device_id=where_to(seq),
                device_id_type=pl.DeviceIdType.MESH,
            )

        found = []
        if origin == "own":
            if level < levels:
                found.append((here & (z < last), copy(level + 1, me + PLANE, own_send.at[0, level, g])))
            found.append((here & needs(level, p, px), copy(level, base + px, own_send.at[1, level, g])))
            found.append((here & needs(level, p, py), copy(level, base + py, own_send.at[2, level, g])))
        elif origin == "x":
            go = here & needs(level, px, py) & (g >= split)
            if level in (0, levels):
                go = go & ((px == 0) | (px == PLANE - 1))
            found.append((go, copy(level, base + py, relay_send.at[0, level, g])))
        elif origin == "y":
            go = here & needs(level, py, px)
            if level in (0, levels):
                go = go & ((g < split) | ((py != 0) & (py != PLANE - 1)))
            else:
                go = go & (g < split)
            found.append((go, copy(level, base + px, relay_send.at[1, level, g])))
        return found

    def have(level, origin):
        held = z >= level
        if origin != "own":
            held = held & needs(level, residue[origin], p)
        return held

    def arrive(level, origin, g):
        if (level, origin) != (0, "own"):
            slot = level * PLANE + residue[origin]

            @pl.when(have(level, origin))
            def _():
                pltpu.make_async_remote_copy(
                    src_ref=buf.at[slot, g],
                    dst_ref=buf.at[slot, g],
                    send_sem=own_send.at[0, 0, 0],
                    recv_sem=recv.at[slot, g],
                    device_id=where_to(base + px),
                    device_id_type=pl.DeviceIdType.MESH,
                ).wait_recv()

        for condition, copy in sends(level, origin, g):
            pl.when(condition)(copy.start)

    def mask_of(slot, causal):
        keys = lax.broadcasted_iota(jnp.int32, (tile, tokens), 0)
        parts = []
        for half in range(tokens // tile):
            part = keys >= rel_ref[pl.ds(slot * (tokens // tile) + half, 1), :]
            if causal:
                part = part & (keys + half * tile <= lax.broadcasted_iota(jnp.int32, (tile, tokens), 1))
            parts.append(part)
        return jnp.concatenate([jnp.where(part, 0.0, NEGATIVE) for part in parts], axis=0)

    def compute(slot, g, first):
        k_tile = buf[slot, g, 0]
        v_tile = jnp.concatenate(
            [buf[slot, g, 1, half * tile:(half + 1) * tile] for half in range(tokens // tile)], axis=1)
        bias = mask_of(slot, first)
        for c in range(group_size):
            h = g * group_size + c
            scores = lax.dot_general(k_tile, q_ref[h], (((1,), (1,)), ((), ())),
                                     preferred_element_type=jnp.float32)
            scores = scores + bias
            new_top = jnp.max(scores, axis=0, keepdims=True)
            if not first:
                old_top = top[h]
                new_top = jnp.maximum(old_top, new_top)
                factor = jnp.exp2((old_top - new_top) * scale)
            weights = jnp.exp2((scores - new_top) * scale)
            weight_sum = jnp.sum(weights, axis=0, keepdims=True)
            summed = lax.dot_general(v_tile, weights.astype(jnp.bfloat16), (((1,), (0,)), ((), ())),
                                     preferred_element_type=jnp.float32)
            top[h] = new_top
            if first:
                total[h] = weight_sum
                acc[h] = summed
            else:
                total[h] = total[h] * factor + weight_sum
                acc[h] = acc[h] * factor + summed

    partner.wait_recv()
    local.wait()
    stages = [
        [(0, "own")],
        [(1, "own"), (0, "x"), (0, "y")],
        [(1, "x"), (1, "y"), (0, "diag"), (2, "own")],
        [(1, "diag"), (2, "x"), (2, "y")],
        [(2, "diag")],
    ]
    everything = [entry for stage in stages for entry in stage]

    def start_own(g, _):
        arrive(0, "own", g)
        return 0

    lax.fori_loop(0, heads, start_own, 0)
    for stage in stages:
        def one_head(g, _):
            for level, origin in stage:
                slot = level * PLANE + residue[origin]
                if (level, origin) == (0, "own"):
                    compute(slot, g, True)
            if stage[0] != (0, "own"):
                for level, origin in stage:
                    arrive(level, origin, g)
                    slot = level * PLANE + residue[origin]
                    pl.when(have(level, origin))(functools.partial(compute, slot, g, False))
            return 0

        lax.fori_loop(0, heads, one_head, 0)

    def finish(h, _):
        o_ref[h] = jnp.transpose(acc[h] / total[h]).astype(o_ref.dtype)
        return 0

    lax.fori_loop(0, q_heads, finish, 0)
    partner.wait_send()

    def sent(g, _):
        for level, origin in everything:
            for condition, copy in sends(level, origin, g):
                pl.when(condition)(copy.wait_send)
        return 0

    lax.fori_loop(0, heads, sent, 0)


def body(groups, queries, keys, values, doc_start, tile_list, tile_count):
    tokens, q_heads, dim = queries.shape
    tile, all_heads, _ = keys.shape
    heads = all_heads // lax.axis_size("head")
    levels = MAXDOC // tokens // PLANE
    slots = (levels + 1) * PLANE
    halves = tokens // tile
    z = lax.axis_index("seq") // PLANE
    slot = jnp.arange(slots, dtype=jnp.int32)
    block = (z - slot // PLANE) * PLANE + slot % PLANE
    ids = (block[:, None] * halves + jnp.arange(halves, dtype=jnp.int32)).reshape(-1)
    live = jnp.arange(tile_list.shape[1], dtype=jnp.int32) < tile_count[0]
    listed = jnp.any((tile_list[0][None, :] == ids[:, None]) & live[None, :], axis=1)
    rel = jnp.where(listed[:, None], doc_start[None, :] - ids[:, None] * tile, FAR)

    vmem = pl.BlockSpec(memory_space=pltpu.VMEM)
    out = pl.pallas_call(
        functools.partial(kernel, groups, levels),
        out_shape=jax.ShapeDtypeStruct((q_heads, tokens, dim), queries.dtype),
        in_specs=[vmem] * 3,
        out_specs=vmem,
        scratch_shapes=[
            pltpu.VMEM((slots, heads, 2, tokens, dim), keys.dtype),
            pltpu.VMEM((q_heads, 1, tokens), jnp.float32),
            pltpu.VMEM((q_heads, 1, tokens), jnp.float32),
            pltpu.VMEM((q_heads, dim, tokens), jnp.float32),
            pltpu.SemaphoreType.DMA,
            pltpu.SemaphoreType.DMA,
            pltpu.SemaphoreType.DMA((3, levels + 1, heads)),
            pltpu.SemaphoreType.DMA((2, levels + 1, heads)),
            pltpu.SemaphoreType.DMA((slots, heads)),
        ],
        compiler_params=pltpu.CompilerParams(
            collective_id=0, has_side_effects=True, vmem_limit_bytes=40 * 1024 * 1024),
    )(rel, queries.transpose(1, 0, 2), jnp.stack([keys.transpose(1, 0, 2), values.transpose(1, 2, 0)], axis=1))
    return out.transpose(1, 0, 2)


def solution(mesh):
    in_specs = (
        P("seq", "head", None),
        P(("seq", "head"), None, None),
        P(("seq", "head"), None, None),
        P("seq"),
        P("seq", None),
        P("seq"),
    )
    return jax.shard_map(
        functools.partial(body, mesh.shape["seq"] // PLANE),
        mesh=mesh, in_specs=in_specs, out_specs=P("seq", "head", None), check_vma=False)
```
